32 devices in a mesh: prow: 8 (over z, core), pcol: 4 (over y, x).
Axes of the slice: x: 2, y: 2, z: 4, core: 2. Of those that a mesh axis runs over, the one named last changes fastest.
Arguments:
- matrix: float32 [8192, 24576], P('prow', 'pcol'), may hold values from -14 to 104.50967, as said below
Outputs:
- factored: float32 [8192, 24576], P('prow', 'pcol')
- tfactors: float32 [2, 128, 128], replicated
The draws below stay inside these ranges and needn't reach their ends.
Inputs may be any that keep to these rules, and one draw needn't show every extreme that they name: `matrix`: real entries.
All inputs are finite; a program needn't handle non-finite values.
Results may differ from the reference program's by a relative error of at most 0.0003.
Values sent between devices are 32-bit elements; how exact they have to be, the bound alone decides.
A program may use at most 192 MiB of HBM per device.

```python
import math
import jax
import jax.numpy as jnp
from jax import lax

NB = 128
NCOL = 24576
ROWS = 8192


def draw_matrix(key, part):
    noise_key = jax.random.fold_in(key, 11)
    base = jax.random.truncated_normal(noise_key, -6.0, 6.0, (ROWS, NCOL), jnp.float32)
    diagonal = (jnp.arange(ROWS)[:, None] == jnp.arange(NCOL)[None, :]).astype(jnp.float32)
    return base + math.sqrt(ROWS) * diagonal


def setup_inputs(seed: int = 0) -> dict:
    streams_of = jax.random.split(jax.random.key(seed), 2)
    return {
        "matrix": draw_matrix(jax.random.fold_in(streams_of[1], 71), 0),
    }


highest = lax.Precision.HIGHEST

def transposed_product(left, right):
    return lax.dot_general(left.astype(jnp.float32), right.astype(jnp.float32), (((0,), (0,)), ((), ())), precision=highest, preferred_element_type=jnp.float32)

def matmul(left, right):
    return jnp.dot(left.astype(jnp.float32), right.astype(jnp.float32), precision=highest, preferred_element_type=jnp.float32)

def householder_panel(panel_cols, first_row):
    row_count = panel_cols.shape[0]
    row_ids = jnp.arange(row_count, dtype=jnp.int32)
    column_ids = jnp.arange(NB, dtype=jnp.int32)

    def single_column(column, carry):
        current, vectors = carry
        column = column.astype(jnp.int32)
        target = (first_row + column).astype(jnp.int32)
        values = lax.dynamic_slice_in_dim(current, column, 1, 1)[:, 0]
        below = jnp.where(row_ids >= target, values, jnp.zeros_like(values))
        length = jnp.sqrt(jnp.sum(below * below))
        leading = lax.dynamic_index_in_dim(values, target, 0, keepdims=False)
        divisor = leading + length
        vector = jnp.where(row_ids == target, jnp.ones_like(below), below / divisor)
        tau_value = divisor / length
        weights = jnp.dot(vector, current, precision=highest) * (column_ids >= column).astype(current.dtype)
        current = current - tau_value * vector[:, None] * weights[None, :]
        vectors = lax.dynamic_update_slice(vectors, vector[:, None], (jnp.int32(0), column))
        return (current, vectors)
    start_vectors = jnp.zeros((row_count, NB), panel_cols.dtype)
    current, vectors = lax.fori_loop(0, NB, single_column, (panel_cols, start_vectors))
    packed_panel = jnp.where(row_ids[:, None] > first_row + column_ids[None, :], vectors, current)
    inner = transposed_product(vectors, vectors)
    inverse_t = jnp.triu(inner, 1) + jnp.diag(jnp.diag(inner)) * 0.5
    identity = jnp.eye(NB, dtype=panel_cols.dtype)
    tfactor = jax.scipy.linalg.solve_triangular(inverse_t, identity, lower=False)
    return (vectors, tfactor, packed_panel)

def reference(matrix):
    column_ids = jnp.arange(NCOL, dtype=jnp.int32)
    leading_reflector_vectors, first_t, leading_packed_panel = householder_panel(matrix[:, :NB], 0)
    first_products = transposed_product(leading_reflector_vectors, matrix)
    first_z = jnp.where((column_ids >= NB)[None, :], matmul(first_t.T, first_products), 0.0)
    second_panel = matrix[:, NB:2 * NB] - matmul(leading_reflector_vectors, first_z[:, NB:2 * NB])
    second_vectors, second_t, following_packed_panel = householder_panel(second_panel, NB)
    coupling = transposed_product(second_vectors, leading_reflector_vectors)
    second_products = transposed_product(second_vectors, matrix) - matmul(coupling, first_z)
    second_z = jnp.where((column_ids >= 2 * NB)[None, :], matmul(second_t.T, second_products), 0.0)
    both_vectors = jnp.concatenate([leading_reflector_vectors, second_vectors], axis=1)
    both_z = jnp.concatenate([first_z, second_z], axis=0)

    def one_block(index, current):
        begin = (index * NB).astype(jnp.int32)
        block_cols = lax.dynamic_slice_in_dim(current, begin, NB, 1)
        block_z = lax.dynamic_slice_in_dim(both_z, begin, NB, 1)
        return lax.dynamic_update_slice(current, block_cols - matmul(both_vectors, block_z), (jnp.int32(0), begin))
    result = lax.fori_loop(0, NCOL // NB, one_block, matrix)
    result = result.at[:, :2 * NB].set(jnp.concatenate([leading_packed_panel, following_packed_panel], axis=1))
    return (result, jnp.stack([first_t, second_t]))
```

```python
import jax
import jax.numpy as jnp
from jax import lax
from jax.experimental import pallas as pl
from jax.experimental.pallas import tpu as pltpu
from jax.sharding import PartitionSpec as P

NB = 128
NP = 2 * NB

highest = lax.Precision.HIGHEST
high = lax.Precision.HIGH


def transposed_product(left, right, precision):
    return lax.dot_general(
        left, right, (((0,), (0,)), ((), ())), precision=precision, preferred_element_type=jnp.float32
    )


def matmul(left, right, precision=highest):
    return jnp.dot(left, right, precision=precision, preferred_element_type=jnp.float32)


def broadcast_first(value, axis, bits):
    size = lax.axis_size(axis)
    value = jnp.where(lax.axis_index(axis) == 0, value, 0.0)
    holders = [0]
    for bit in bits:
        pairs = [(i, i + bit) for i in holders if i + bit < size]
        value = value + lax.ppermute(value, axis, pairs)
        holders = holders + [target for _, target in pairs]
    return value


def identity_tile():
    rows = lax.broadcasted_iota(jnp.int32, (NB, NB), 0)
    cols = lax.broadcasted_iota(jnp.int32, (NB, NB), 1)
    return jnp.where(rows == cols, 1.0, 0.0)


def eliminate(systems):
    row_ids = lax.broadcasted_iota(jnp.int32, (NB, NB), 0)
    lane_ids = lax.broadcasted_iota(jnp.int32, (NB, NB), 1)
    for _, w_ref in systems:
        w_ref[...] = jnp.where(row_ids == lane_ids, 1.0, 0.0)

    def step(k, carry):
        for x_ref, w_ref in systems:
            x = x_ref[...]
            pivot_row = x_ref[pl.ds(k, 1), :]
            pivot_w = w_ref[pl.ds(k, 1), :]
            pick = lane_ids == k
            pivot = jnp.sum(jnp.where(pick[:1], pivot_row, 0.0), axis=1, keepdims=True)
            inverse = 1.0 / pivot
            column = jnp.sum(jnp.where(pick & (row_ids > k), x, 0.0), axis=1, keepdims=True)
            x_ref[...] = x - column * (pivot_row * inverse)
            w_ref[...] = w_ref[...] - column * (pivot_w * inverse)
        return carry

    lax.fori_loop(0, NB, step, 0)


def diagonal_column(x):
    return jnp.sum(x * identity_tile(), axis=1, keepdims=True)


def cholesky_kernel(gram_ref, upper_ref, inverse_ref, x_ref, w_ref):
    row_ids = lax.broadcasted_iota(jnp.int32, (NB, NB), 0)
    lane_ids = lax.broadcasted_iota(jnp.int32, (NB, NB), 1)
    lead, tail = pl.ds(0, NB), pl.ds(NB, NB)
    zero = jnp.zeros((NB, NB), jnp.float32)

    def block():
        eliminate([(x_ref, w_ref)])
        x = x_ref[...]
        scale = 1.0 / jnp.sqrt(diagonal_column(x))
        return jnp.where(row_ids <= lane_ids, x, 0.0) * scale, w_ref[...] * scale

    x_ref[...] = gram_ref[lead, lead]
    r00, i00 = block()
    upper_ref[lead, lead] = r00
    inverse_ref[lead, lead] = i00
    r01 = matmul(i00, gram_ref[lead, tail])
    upper_ref[lead, tail] = r01
    r01_t = r01.T
    x_ref[...] = gram_ref[tail, tail] - matmul(r01_t, r01)
    r11, i11 = block()
    upper_ref[tail, tail] = r11
    inverse_ref[tail, tail] = i11
    upper_ref[tail, lead] = zero
    inverse_ref[lead, tail] = zero
    inverse_ref[tail, lead] = -matmul(i11, matmul(r01_t, inverse_ref[lead, lead]))


def lower_upper_kernel(
    top_ref, upper_ref, inverse_ref, lower_ref, packed_ref, left_ref, right_ref, t_ref,
    s_ref, st_ref, li_ref, ui_ref, x_ref, w_ref, xt_ref, wt_ref,
):
    row_ids = lax.broadcasted_iota(jnp.int32, (NB, NB), 0)
    lane_ids = lax.broadcasted_iota(jnp.int32, (NB, NB), 1)
    lead, tail = pl.ds(0, NB), pl.ds(NB, NB)
    zero = jnp.zeros((NB, NB), jnp.float32)
    eye = identity_tile()
    s_ref[...] = matmul(top_ref[...], inverse_ref[...].T)
    s_ref[lead, lead] = s_ref[lead, lead] + eye
    s_ref[tail, tail] = s_ref[tail, tail] + eye
    st_ref[...] = s_ref[...].T

    def block(which, index):
        eliminate([(x_ref, w_ref), (xt_ref, wt_ref)])
        upper = jnp.where(row_ids <= lane_ids, x_ref[...], 0.0)
        xt = xt_ref[...]
        scale = 1.0 / diagonal_column(xt)
        lower_t = jnp.where(row_ids < lane_ids, xt * scale, eye)
        lower_ref[which, which] = lower_t.T
        li_ref[which, which] = w_ref[...]
        ui_ref[which, which] = wt_ref[...] * scale
        t_ref[index] = matmul(upper, w_ref[...].T)

    x_ref[...] = s_ref[lead, lead]
    xt_ref[...] = st_ref[lead, lead]
    block(lead, 0)
    u01 = matmul(li_ref[lead, lead], s_ref[lead, tail])
    l10_t = matmul(ui_ref[lead, lead], st_ref[lead, tail])
    l10, u01_t = l10_t.T, u01.T
    lower_ref[tail, lead] = l10
    lower_ref[lead, tail] = zero
    li_ref[lead, tail] = zero
    ui_ref[lead, tail] = zero
    li_ref[tail, lead] = matmul(l10, li_ref[lead, lead])
    ui_ref[tail, lead] = matmul(u01_t, ui_ref[lead, lead])
    corner = s_ref[tail, tail] - matmul(l10, u01)
    x_ref[...] = corner
    xt_ref[...] = corner.T
    block(tail, 1)
    li_ref[tail, lead] = -matmul(li_ref[tail, tail], li_ref[tail, lead])
    ui_ref[tail, lead] = -matmul(ui_ref[tail, tail], ui_ref[tail, lead])
    left_ref[...] = matmul(li_ref[...], inverse_ref[...])
    right_ref[...] = matmul(ui_ref[...], inverse_ref[...]).T
    all_rows = lax.broadcasted_iota(jnp.int32, (NP, NP), 0)
    all_lanes = lax.broadcasted_iota(jnp.int32, (NP, NP), 1)
    packed_ref[...] = jnp.where(all_rows <= all_lanes, -upper_ref[...], lower_ref[...])


def in_vmem(count):
    return [pl.BlockSpec(memory_space=pltpu.VMEM)] * count


def cholesky(gram):
    square = jax.ShapeDtypeStruct((NP, NP), jnp.float32)
    return pl.pallas_call(
        cholesky_kernel,
        name="cholesky",
        out_shape=(square, square),
        in_specs=in_vmem(1),
        out_specs=tuple(in_vmem(2)),
        scratch_shapes=[pltpu.VMEM((NB, NB), jnp.float32)] * 2,
        cost_estimate=pl.CostEstimate(flops=10**9, bytes_accessed=10**8, transcendentals=0),
    )(gram)


def lower_upper(top, upper, inverse):
    square = jax.ShapeDtypeStruct((NP, NP), jnp.float32)
    return pl.pallas_call(
        lower_upper_kernel,
        name="lower_upper",
        out_shape=(square,) * 4 + (jax.ShapeDtypeStruct((2, NB, NB), jnp.float32),),
        in_specs=in_vmem(3),
        out_specs=tuple(in_vmem(5)),
        scratch_shapes=[pltpu.VMEM((NP, NP), jnp.float32)] * 4
        + [pltpu.VMEM((NB, NB), jnp.float32)] * 4,
        cost_estimate=pl.CostEstimate(flops=10**9, bytes_accessed=10**8, transcendentals=0),
    )(top, upper, inverse)


def per_device(matrix):
    rows_dev = matrix.shape[0]
    my_row = lax.axis_index("prow")
    my_col = lax.axis_index("pcol")
    first = my_row == 0
    panel = matrix[:, :NP]
    gram_local = transposed_product(panel, panel, highest)
    top_local = jnp.where(first, panel[:NP], 0.0)
    both = jnp.where(my_col == 0, jnp.concatenate([gram_local, top_local], axis=0), 0.0)
    both = lax.psum(both, ("prow", "pcol"))
    bits = []
    while 2 ** len(bits) < lax.axis_size("pcol"):
        bits.append(2 ** len(bits))
    half = rows_dev // 2
    panel = jnp.concatenate(
        [
            broadcast_first(panel[:half], "pcol", bits),
            broadcast_first(panel[half:], "pcol", bits[::-1]),
        ],
        axis=0,
    )
    upper, inverse = cholesky(both[:NP])
    shifted = panel.at[:NP].add(jnp.where(first, upper, 0.0))
    products = lax.psum(transposed_product(shifted, matrix, high), "prow")
    lower, packed_top, left, right, tfactors = lower_upper(both[NP:], upper, inverse)
    reflectors = matmul(shifted, right)
    packed = reflectors.at[:NP].set(jnp.where(first, packed_top, reflectors[:NP]))
    reflectors = reflectors.at[:NP].set(jnp.where(first, lower, reflectors[:NP]))
    weights = matmul(left, products, high)
    result = matrix - matmul(reflectors, weights, high)
    result = result.at[:, :NP].set(jnp.where(my_col == 0, packed, result[:, :NP]))
    return (result, tfactors)


def solution(mesh):
    return jax.shard_map(
        per_device,
        mesh=mesh,
        in_specs=(P("prow", "pcol"),),
        out_specs=(P("prow", "pcol"), P()),
        check_vma=False,
    )
```

```python
import jax
import jax.numpy as jnp
from jax import lax
from jax.experimental import pallas as pl
from jax.experimental.pallas import tpu as pltpu
from jax.sharding import PartitionSpec as P

NB = 128
NP = 2 * NB

highest = lax.Precision.HIGHEST
high = lax.Precision.HIGH


def transposed_product(left, right, precision):
    return lax.dot_general(
        left, right, (((0,), (0,)), ((), ())), precision=precision, preferred_element_type=jnp.float32
    )


def matmul(left, right, precision=highest):
    return jnp.dot(left, right, precision=precision, preferred_element_type=jnp.float32)


def broadcast_first(value, axis, bits):
    size = lax.axis_size(axis)
    value = jnp.where(lax.axis_index(axis) == 0, value, 0.0)
    holders = [0]
    for bit in bits:
        pairs = [(i, i + bit) for i in holders if i + bit < size]
        value = value + lax.ppermute(value, axis, pairs)
        holders = holders + [target for _, target in pairs]
    return value


def doublings(axis):
    bits = []
    while 2 ** len(bits) < lax.axis_size(axis):
        bits.append(2 ** len(bits))
    return bits


def butterfly_sum(value, axis):
    size = lax.axis_size(axis)
    if size & (size - 1):
        return lax.psum(value, axis)
    for bit in doublings(axis):
        value = value + lax.ppermute(value, axis, [(i, i ^ bit) for i in range(size)])
    return value


def identity_tile():
    rows = lax.broadcasted_iota(jnp.int32, (NB, NB), 0)
    cols = lax.broadcasted_iota(jnp.int32, (NB, NB), 1)
    return jnp.where(rows == cols, 1.0, 0.0)


def eliminate(systems):
    row_ids = lax.broadcasted_iota(jnp.int32, (NB, NB), 0)
    lane_ids = lax.broadcasted_iota(jnp.int32, (NB, NB), 1)
    for _, w_ref in systems:
        w_ref[...] = jnp.where(row_ids == lane_ids, 1.0, 0.0)

    def step(k, carry):
        for x_ref, w_ref in systems:
            x = x_ref[...]
            pivot_row = x_ref[pl.ds(k, 1), :]
            pivot_w = w_ref[pl.ds(k, 1), :]
            pick = lane_ids == k
            pivot = jnp.sum(jnp.where(pick[:1], pivot_row, 0.0), axis=1, keepdims=True)
            inverse = 1.0 / pivot
            column = jnp.sum(jnp.where(pick & (row_ids > k), x, 0.0), axis=1, keepdims=True)
            x_ref[...] = x - column * (pivot_row * inverse)
            w_ref[...] = w_ref[...] - column * (pivot_w * inverse)
        return carry

    lax.fori_loop(0, NB, step, 0)


def diagonal_column(x):
    return jnp.sum(x * identity_tile(), axis=1, keepdims=True)


def cholesky_kernel(gram_ref, upper_ref, inverse_ref, x_ref, w_ref):
    row_ids = lax.broadcasted_iota(jnp.int32, (NB, NB), 0)
    lane_ids = lax.broadcasted_iota(jnp.int32, (NB, NB), 1)
    lead, tail = pl.ds(0, NB), pl.ds(NB, NB)
    zero = jnp.zeros((NB, NB), jnp.float32)

    def block():
        eliminate([(x_ref, w_ref)])
        x = x_ref[...]
        scale = 1.0 / jnp.sqrt(diagonal_column(x))
        return jnp.where(row_ids <= lane_ids, x, 0.0) * scale, w_ref[...] * scale

    x_ref[...] = gram_ref[lead, lead]
    r00, i00 = block()
    upper_ref[lead, lead] = r00
    inverse_ref[lead, lead] = i00
    r01 = matmul(i00, gram_ref[lead, tail])
    upper_ref[lead, tail] = r01
    r01_t = r01.T
    x_ref[...] = gram_ref[tail, tail] - matmul(r01_t, r01)
    r11, i11 = block()
    upper_ref[tail, tail] = r11
    inverse_ref[tail, tail] = i11
    upper_ref[tail, lead] = zero
    inverse_ref[lead, tail] = zero
    inverse_ref[tail, lead] = -matmul(i11, matmul(r01_t, inverse_ref[lead, lead]))


def lower_upper_kernel(
    top_ref, upper_ref, inverse_ref, lower_ref, packed_ref, left_ref, right_ref, t_ref,
    s_ref, st_ref, li_ref, ui_ref, x_ref, w_ref, xt_ref, wt_ref,
):
    row_ids = lax.broadcasted_iota(jnp.int32, (NB, NB), 0)
    lane_ids = lax.broadcasted_iota(jnp.int32, (NB, NB), 1)
    lead, tail = pl.ds(0, NB), pl.ds(NB, NB)
    zero = jnp.zeros((NB, NB), jnp.float32)
    eye = identity_tile()
    s_ref[...] = matmul(top_ref[...], inverse_ref[...].T)
    s_ref[lead, lead] = s_ref[lead, lead] + eye
    s_ref[tail, tail] = s_ref[tail, tail] + eye
    st_ref[...] = s_ref[...].T

    def block(which, index):
        eliminate([(x_ref, w_ref), (xt_ref, wt_ref)])
        upper = jnp.where(row_ids <= lane_ids, x_ref[...], 0.0)
        xt = xt_ref[...]
        scale = 1.0 / diagonal_column(xt)
        lower_t = jnp.where(row_ids < lane_ids, xt * scale, eye)
        lower_ref[which, which] = lower_t.T
        li_ref[which, which] = w_ref[...]
        ui_ref[which, which] = wt_ref[...] * scale
        t_ref[index] = matmul(upper, w_ref[...].T)

    x_ref[...] = s_ref[lead, lead]
    xt_ref[...] = st_ref[lead, lead]
    block(lead, 0)
    u01 = matmul(li_ref[lead, lead], s_ref[lead, tail])
    l10_t = matmul(ui_ref[lead, lead], st_ref[lead, tail])
    l10, u01_t = l10_t.T, u01.T
    lower_ref[tail, lead] = l10
    lower_ref[lead, tail] = zero
    li_ref[lead, tail] = zero
    ui_ref[lead, tail] = zero
    li_ref[tail, lead] = matmul(l10, li_ref[lead, lead])
    ui_ref[tail, lead] = matmul(u01_t, ui_ref[lead, lead])
    corner = s_ref[tail, tail] - matmul(l10, u01)
    x_ref[...] = corner
    xt_ref[...] = corner.T
    block(tail, 1)
    li_ref[tail, lead] = -matmul(li_ref[tail, tail], li_ref[tail, lead])
    ui_ref[tail, lead] = -matmul(ui_ref[tail, tail], ui_ref[tail, lead])
    left_ref[...] = matmul(li_ref[...], inverse_ref[...])
    right_ref[...] = matmul(ui_ref[...], inverse_ref[...]).T
    all_rows = lax.broadcasted_iota(jnp.int32, (NP, NP), 0)
    all_lanes = lax.broadcasted_iota(jnp.int32, (NP, NP), 1)
    packed_ref[...] = jnp.where(all_rows <= all_lanes, -upper_ref[...], lower_ref[...])


def in_vmem(count):
    return [pl.BlockSpec(memory_space=pltpu.VMEM)] * count


def cholesky(gram):
    square = jax.ShapeDtypeStruct((NP, NP), jnp.float32)
    return pl.pallas_call(
        cholesky_kernel,
        name="cholesky",
        out_shape=(square, square),
        in_specs=in_vmem(1),
        out_specs=tuple(in_vmem(2)),
        scratch_shapes=[pltpu.VMEM((NB, NB), jnp.float32)] * 2,
        cost_estimate=pl.CostEstimate(flops=10**9, bytes_accessed=10**8, transcendentals=0),
    )(gram)


def lower_upper(top, upper, inverse):
    square = jax.ShapeDtypeStruct((NP, NP), jnp.float32)
    return pl.pallas_call(
        lower_upper_kernel,
        name="lower_upper",
        out_shape=(square,) * 4 + (jax.ShapeDtypeStruct((2, NB, NB), jnp.float32),),
        in_specs=in_vmem(3),
        out_specs=tuple(in_vmem(5)),
        scratch_shapes=[pltpu.VMEM((NP, NP), jnp.float32)] * 4
        + [pltpu.VMEM((NB, NB), jnp.float32)] * 4,
        cost_estimate=pl.CostEstimate(flops=10**9, bytes_accessed=10**8, transcendentals=0),
    )(top, upper, inverse)


def per_device(matrix):
    rows_dev = matrix.shape[0]
    my_row = lax.axis_index("prow")
    my_col = lax.axis_index("pcol")
    first = my_row == 0
    panel = matrix[:, :NP]
    bits = doublings("pcol")
    half = rows_dev // 2
    panel = jnp.concatenate(
        [
            broadcast_first(panel[:half], "pcol", bits),
            broadcast_first(panel[half:], "pcol", bits[::-1]),
        ],
        axis=0,
    )
    gram = butterfly_sum(transposed_product(panel, panel, highest), "prow")
    top = broadcast_first(panel[:NP], "prow", doublings("prow")[::-1])
    upper, inverse = cholesky(gram)
    shifted = panel.at[:NP].add(jnp.where(first, upper, 0.0))
    products = lax.psum(transposed_product(shifted, matrix, high), "prow")
    lower, packed_top, left, right, tfactors = lower_upper(top, upper, inverse)
    reflectors = matmul(shifted, right)
    packed = reflectors.at[:NP].set(jnp.where(first, packed_top, reflectors[:NP]))
    reflectors = reflectors.at[:NP].set(jnp.where(first, lower, reflectors[:NP]))
    weights = matmul(left, products, high)
    result = matrix - matmul(reflectors, weights, high)
    result = result.at[:, :NP].set(jnp.where(my_col == 0, packed, result[:, :NP]))
    return (result, tfactors)


def solution(mesh):
    return jax.shard_map(
        per_device,
        mesh=mesh,
        in_specs=(P("prow", "pcol"),),
        out_specs=(P("prow", "pcol"), P()),
        check_vma=False,
    )
```
